32 devices in a mesh: dp: 4 (over x, y), tp: 8 (over z, core).
Axes of the slice: x: 2, y: 2, z: 4, core: 2. Of those that a mesh axis runs over, the one named last changes fastest.
Arguments:
- x: bfloat16 [8192, 8192], P('dp'), parts along dimension 0
- w_gate: bfloat16 [8192, 32768], P(None, 'tp')
- w_up: bfloat16 [8192, 32768], P(None, 'tp')
- w_down: bfloat16 [32768, 8192], P('tp')
Outputs:
- output: bfloat16 [8192, 8192], P('dp'), parts along dimension 0
There are 4 independent parts. The reference program is written for one: setup_inputs(seed, part) draws one part's arguments, and reference() takes and returns one part's arrays. A program takes and returns all parts, laid end to end along the dimension named above; an argument that names none is the same for every part.
All inputs are finite; a program needn't handle non-finite values.
Results may differ from the reference program's by a relative error of at most 0.016.
Values are sent between devices in bfloat16 or wider.
A program may use at most 2 GiB of HBM per device.

```python
import jax
import jax.numpy as jnp

ROWS = 2048
D = 8192
FF = 32768


def setup_inputs(seed: int = 0, part: int = 0) -> dict:
    kx, kg, ku, kd = jax.random.split(jax.random.key(seed), 4)
    drawn = {
        "x": jax.random.normal(jax.random.fold_in(kx, part), (ROWS, D), jnp.float32),
        "w_gate": jax.random.normal(kg, (D, FF), jnp.float32) * D**-0.5,
        "w_up": jax.random.normal(ku, (D, FF), jnp.float32) * D**-0.5,
        "w_down": jax.random.normal(kd, (FF, D), jnp.float32) * FF**-0.5,
    }
    return {k: v.astype(jnp.bfloat16) for k, v in drawn.items()}


def reference(x, w_gate, w_up, w_down):
    gate = jnp.dot(x, w_gate, preferred_element_type=jnp.float32)
    up = jnp.dot(x, w_up, preferred_element_type=jnp.float32)
    hidden = (jax.nn.silu(gate) * up).astype(jnp.bfloat16)
    return jnp.dot(hidden, w_down, preferred_element_type=jnp.float32).astype(jnp.bfloat16)
```

```python
import functools

import jax
import jax.numpy as jnp
from jax import lax
from jax.experimental import pallas as pl
from jax.experimental.pallas import tpu as pltpu
from jax.sharding import PartitionSpec as P

MESH = pl.DeviceIdType.MESH
BF16, F32 = jnp.bfloat16, jnp.float32

T = 256
R = 256
H = R // 2
BIG, SMALL = 512, 256
NBIG, NSMALL = 3, 2
N_OWN, N_PRECV, N_RO, N_RI, N_PS, N_AS, N_FS, N_Y = 17, 14, 14, 12, 4, 8, 8, 24
LAG_P, LAG_AO, LAG_AI, LAG_F, LAG_Y1, LAG_Y2 = 4, 4, 9, 14, 19, 24


def kernel(
    d, f, x, wg, wu, wd, y,
    xb, hid, wgu, wdb, gu, own, precv, ro, ri, ps, asd, fs,
    wsem, xsem, ps_sem, precv_sem, as_sem, ro_sem, ri_sem, fs_sem, ya_sem, yb_sem, yp_sem, fw_sem,
):
    half = d // 2
    steps = f // T
    assert half // T == steps
    n_units = steps * (NBIG * BIG + NSMALL * SMALL) // R
    per_big = BIG // R
    big_units = NBIG * steps * per_big

    tp = lax.axis_index("tp")
    z, c = lax.div(tp, 2), lax.rem(tp, 2)
    inner = jnp.logical_and(z >= 1, z <= 2)
    outer = jnp.logical_not(inner)
    partner = {"tp": z * 2 + 1 - c}
    near = 1 + lax.div(z, 2)
    to_near = {"tp": near * 2 + c}
    to_inner = {"tp": (3 - near) * 2 + c}
    to_outer = {"tp": 3 * (near - 1) * 2 + c}
    near_rows = (near - 1) * H
    far_rows = (2 - near) * H
    my_cols, other_cols = c * half, (1 - c) * half

    def remote(src, dst, send, recv, dev):
        return pltpu.make_async_remote_copy(
            src_ref=src, dst_ref=dst, send_sem=send, recv_sem=recv, device_id=dev, device_id_type=MESH
        )

    def valid(v):
        return jnp.logical_and(v >= 0, v < n_units)

    def slot(v, n):
        return jnp.where(valid(v), lax.rem(v + 64 * n, n), n)

    def unit_at(v):
        b = jnp.where(v < big_units, 1, 0)
        w = v - big_units
        row_b = lax.div(v, steps * per_big) * BIG + lax.rem(v, per_big) * R
        col_b = lax.div(lax.rem(v, steps * per_big), per_big) * T
        row_s = NBIG * BIG + lax.div(w, steps) * SMALL
        col_s = lax.rem(w, steps) * T
        row = b * row_b + (1 - b) * row_s
        col = b * col_b + (1 - b) * col_s
        return row, col

    def y_at(v, rows):
        row, col = unit_at(v)
        return y.at[pl.ds(pl.multiple_of(row + rows, H), H), pl.ds(pl.multiple_of(my_cols + col, T), T)]

    def g_copies(j, s):
        cols = pl.ds(pl.multiple_of(j * T, T), T)
        return [
            pltpu.make_async_copy(wg.at[:, cols], wgu.at[s, :, pl.ds(0, T)], wsem.at[s, 0]),
            pltpu.make_async_copy(wu.at[:, cols], wgu.at[s, :, pl.ds(T, T)], wsem.at[s, 1]),
        ]

    def d_copies(j, s):
        theirs = pl.ds(pl.multiple_of(other_cols + j * T, T), T)
        mine = pl.ds(pl.multiple_of(my_cols + j * T, T), T)
        return [
            pltpu.make_async_copy(wd.at[:, theirs], wdb.at[s, :, pl.ds(0, T)], wsem.at[s, 2]),
            pltpu.make_async_copy(wd.at[:, mine], wdb.at[s, :, pl.ds(T, T)], wsem.at[s, 3]),
        ]

    def x_copy(row, rows, s):
        return pltpu.make_async_copy(x.at[pl.ds(row, rows)], xb.at[s, pl.ds(0, rows)], xsem.at[s])

    def start(copies):
        for cp in copies:
            cp.start()

    def wait(copies):
        for cp in copies:
            cp.wait()

    def ps_copy(v):
        s = lax.rem(v, N_PS)
        return remote(ps.at[s], precv.at[lax.rem(v, N_PRECV)], ps_sem.at[s], precv_sem.at[lax.rem(v, N_PRECV)], partner)

    def ps_free(v):
        @pl.when(v >= N_PS)
        def _():
            ps_copy(v - N_PS).wait_send()

    def p_wait(v):
        @pl.when(valid(v))
        def _():
            ps_copy(v).wait_recv()

    def ao_copy(v):
        s = lax.rem(v, N_AS)
        return remote(asd.at[s], ro.at[lax.rem(v, N_RO)], as_sem.at[s], ro_sem.at[lax.rem(v, N_RO)], to_near)

    def ai_copy(v):
        s = lax.rem(v, N_AS)
        rows = pl.ds(pl.multiple_of(far_rows, H), H)
        return remote(asd.at[s, rows], ri.at[lax.rem(v, N_RI)], as_sem.at[s], ri_sem.at[lax.rem(v, N_RI)], to_inner)

    def a_wait(vo, vi):
        @pl.when(jnp.logical_and(outer, jnp.logical_and(vo >= N_AS, vo < n_units)))
        def _():
            ao_copy(vo - N_AS).wait_send()

        @pl.when(jnp.logical_and(inner, jnp.logical_and(vi >= N_AS, vi < n_units)))
        def _():
            ai_copy(vi - N_AS).wait_send()

        @pl.when(jnp.logical_and(inner, valid(vi)))
        def _():
            ao_copy(vi).wait_recv()

    def a_compute(vo, vi):
        v = jnp.where(inner, vi, vo)
        so = slot(v, N_OWN)
        sr = jnp.where(inner, slot(v, N_RO), N_RO)
        total = own[so] + precv[slot(v, N_PRECV)].astype(F32) + ro[sr].astype(F32)
        own[so] = total
        asd[slot(v, N_AS)] = total.astype(BF16)

    def a_start(vo, vi):
        @pl.when(jnp.logical_and(outer, valid(vo)))
        def _():
            ao_copy(vo).start()

        @pl.when(jnp.logical_and(inner, valid(vi)))
        def _():
            ai_copy(vi).start()

    def f_copies(v):
        s = lax.rem(v, N_FS)
        at = y_at(v, near_rows)
        ys = lax.rem(v, N_Y)
        return [
            remote(fs.at[s], at, fs_sem.at[s, 0], ya_sem.at[ys], to_outer),
            remote(fs.at[s], at, fs_sem.at[s, 1], ya_sem.at[ys], to_inner),
            remote(fs.at[s], at, fs_sem.at[s, 2], yp_sem, partner),
            pltpu.make_async_copy(fs.at[s], at, fs_sem.at[s, 3]),
        ]

    def f_wait_sends(v):
        copies = f_copies(v)
        for cp in copies[:3]:
            cp.wait_send()
        copies[3].wait()

    def f_wait(v):
        @pl.when(jnp.logical_and(inner, jnp.logical_and(v >= N_FS, v < n_units)))
        def _():
            f_wait_sends(v - N_FS)

        @pl.when(jnp.logical_and(inner, valid(v)))
        def _():
            ai_copy(v).wait_recv()

    def f_compute(v):
        v = jnp.where(inner, v, -1)
        rows = pl.ds(pl.multiple_of(near_rows, H), H)
        fs[slot(v, N_FS)] = (own[slot(v, N_OWN), rows, :] + ri[slot(v, N_RI)].astype(F32)).astype(BF16)

    def f_start(v):
        @pl.when(jnp.logical_and(inner, valid(v)))
        def _():
            start(f_copies(v))

    def y1(v):
        @pl.when(jnp.logical_and(inner, valid(v)))
        def _():
            at = y_at(v, far_rows)
            remote(at, at, fw_sem, ya_sem.at[lax.rem(v, N_Y)], to_inner).wait_recv()
            remote(at, at, fw_sem, yb_sem.at[lax.rem(v, N_Y)], to_outer).start()
            remote(at, at, fw_sem, yp_sem, partner).start()

        @pl.when(jnp.logical_and(outer, valid(v)))
        def _():
            at = y_at(v, near_rows)
            remote(at, at, fw_sem, ya_sem.at[lax.rem(v, N_Y)], to_near).wait_recv()
            remote(at, at, fw_sem, yp_sem, partner).start()

    def y2(v):
        @pl.when(jnp.logical_and(outer, valid(v)))
        def _():
            at = y_at(v, far_rows)
            remote(at, at, fw_sem, yb_sem.at[lax.rem(v, N_Y)], to_near).wait_recv()
            remote(at, at, fw_sem, yp_sem, partner).start()

    def waits(u0, r):
        for i in range(r):
            p_wait(u0 - LAG_P + i)
        for i in range(r):
            a_wait(u0 - LAG_AO + i, u0 - LAG_AI + i)
        for i in range(r):
            f_wait(u0 - LAG_F + i)
        for i in range(r):
            y1(u0 - LAG_Y1 + i)
        for i in range(r):
            y2(u0 - LAG_Y2 + i)

    def computes(u0, r):
        for i in range(r):
            a_compute(u0 - LAG_AO + i, u0 - LAG_AI + i)
        for i in range(r):
            f_compute(u0 - LAG_F + i)

    def starts(u0, r):
        for i in range(r):
            a_start(u0 - LAG_AO + i, u0 - LAG_AI + i)
        for i in range(r):
            f_start(u0 - LAG_F + i)

    def epilogue(rows, s, j):
        g, u = gu[pl.ds(0, rows), pl.ds(0, T)], gu[pl.ds(0, rows), pl.ds(T, T)]
        h = (g * jax.nn.sigmoid(g) * u).astype(BF16)
        hid[s, pl.ds(0, rows), pl.ds(pl.multiple_of(j * T, T), T)] = h

    def gate_up(rows, s, w):
        gu[pl.ds(0, rows), :] = jnp.dot(xb[s, pl.ds(0, rows)], wgu[w], preferred_element_type=F32)

    def down(rows, s, w, u0):
        t = jnp.dot(hid[s, pl.ds(0, rows)], wdb[w], preferred_element_type=F32)
        for i in range(rows // R):
            part = t[i * R : (i + 1) * R]
            ps[lax.rem(u0 + i, N_PS)] = part[:, :T].astype(BF16)
            own[lax.rem(u0 + i, N_OWN)] = part[:, T:]

    barrier = pltpu.get_barrier_semaphore()
    x_copy(0, BIG, 0).start()
    start(g_copies(0, 0))
    pl.semaphore_signal(barrier, inc=1, device_id=partner, device_id_type=MESH)

    @pl.when(outer)
    def _():
        pl.semaphore_signal(barrier, inc=1, device_id=to_near, device_id_type=MESH)

    @pl.when(inner)
    def _():
        pl.semaphore_signal(barrier, inc=1, device_id=to_outer, device_id_type=MESH)
        pl.semaphore_signal(barrier, inc=1, device_id=to_inner, device_id_type=MESH)

    gu[...] = jnp.zeros_like(gu)
    ro[N_RO] = jnp.zeros((R, T), BF16)
    x_copy(0, BIG, 0).wait()

    def first(j, _):
        w = lax.rem(j, 2)

        @pl.when(j < steps - 1)
        def _():
            start(g_copies(j + 1, 1 - w))

        @pl.when(j == steps - 1)
        def _():
            start(g_copies(0, 1 - w))
            start(d_copies(0, 1 - w))

        @pl.when(j == 1)
        def _():
            x_copy(BIG, BIG, 1).start()

        wait(g_copies(j, w))
        epilogue(BIG, 0, lax.rem(j + steps - 1, steps))
        gate_up(BIG, 0, w)
        return 0

    lax.fori_loop(0, steps, first, 0)

    @pl.when(outer)
    def _():
        pl.semaphore_wait(barrier, 2)

    @pl.when(inner)
    def _():
        pl.semaphore_wait(barrier, 3)

    def both(t, _):
        k, j = lax.div(t, steps), lax.rem(t, steps)
        w = lax.rem(t, 2)
        sd, sg = lax.rem(k, 2), lax.rem(k + 1, 2)
        u0 = t * per_big
        jn = lax.rem(j + 1, steps)
        start(g_copies(jn, 1 - w))
        start(d_copies(jn, 1 - w))

        @pl.when(j == 0)
        def _():
            x_copy(0, BIG, sg).wait()

        for kk in range(NBIG - 1):
            rows = BIG if kk + 2 < NBIG else SMALL

            @pl.when(t == kk * steps + 1)
            def _():
                x_copy((kk + 2) * BIG, rows, kk % 2).start()

        for i in range(per_big):
            ps_free(u0 + i)
        waits(u0, per_big)
        wait(g_copies(j, w))
        wait(d_copies(j, w))
        epilogue(BIG, jnp.where(j == 0, sd, sg), lax.rem(j + steps - 1, steps))
        computes(u0, per_big)
        gate_up(BIG, sg, w)
        down(BIG, sd, w, u0)
        for i in range(per_big):
            ps_copy(u0 + i).start()
        starts(u0, per_big)
        return 0

    lax.fori_loop(0, steps * (NBIG - 1), both, 0)

    for k in range(NBIG - 1, NBIG + NSMALL - 1):
        rows = BIG if k < NBIG else SMALL
        r = rows // R
        base = (NBIG - 1) * steps * per_big if k < NBIG else big_units + (k - NBIG) * steps
        sd, sg = k % 2, (k + 1) % 2
        last = k == NBIG + NSMALL - 2
        x_copy(0, SMALL, sg).wait()

        def small(j, _, rows=rows, r=r, base=base, sd=sd, sg=sg, last=last, k=k):
            w = lax.rem(j, 2)
            u0 = base + j * r
            jn = lax.rem(j + 1, steps)
            if last:

                @pl.when(j < steps - 1)
                def _():
                    start(g_copies(jn, 1 - w))
            else:
                start(g_copies(jn, 1 - w))
            start(d_copies(jn, 1 - w))
            if not last:

                @pl.when(j == 1)
                def _():
                    x_copy(NBIG * BIG + (k + 2 - NBIG) * SMALL, SMALL, sd).start()

            for i in range(r):
                ps_free(u0 + i)
            waits(u0, r)
            wait(g_copies(j, w))
            wait(d_copies(j, w))
            epilogue(rows, jnp.where(j == 0, sd, sg), lax.rem(j + steps - 1, steps))
            computes(u0, r)
            gate_up(SMALL, sg, w)
            down(rows, sd, w, u0)
            for i in range(r):
                ps_copy(u0 + i).start()
            starts(u0, r)
            return 0

        lax.fori_loop(0, steps, small, 0)

    sd = (NBIG + NSMALL - 1) % 2
    epilogue(SMALL, sd, steps - 1)

    def final(j, _):
        w = lax.rem(j, 2)
        u0 = n_units - steps + j

        @pl.when(j < steps - 1)
        def _():
            start(d_copies(j + 1, 1 - w))

        ps_free(u0)
        waits(u0, 1)
        wait(d_copies(j, w))
        computes(u0, 1)
        down(SMALL, sd, w, u0)
        ps_copy(u0).start()
        starts(u0, 1)
        return 0

    lax.fori_loop(0, steps, final, 0)

    def drain(i, _):
        u0 = n_units + i
        waits(u0, 1)
        computes(u0, 1)
        starts(u0, 1)
        return 0

    lax.fori_loop(0, LAG_Y2, drain, 0)

    for v in range(n_units - N_PS, n_units):
        ps_copy(v).wait_send()

    @pl.when(outer)
    def _():
        for v in range(n_units - N_AS, n_units):
            ao_copy(v).wait_send()

    @pl.when(inner)
    def _():
        for v in range(n_units - N_AS, n_units):
            ai_copy(v).wait_send()
        for v in range(n_units - N_FS, n_units):
            f_wait_sends(v)

    sent = y.at[:, pl.ds(pl.multiple_of(my_cols, T), half)]
    got = y.at[:, pl.ds(pl.multiple_of(other_cols, T), half)]
    remote(sent, got, fw_sem, yp_sem, partner).wait_send()
    remote(sent, got, fw_sem, yp_sem, partner).wait_recv()


def solution(mesh):
    def step(x, w_gate, w_up, w_down):
        d, f = w_gate.shape
        rows = x.shape[0]
        assert rows == NBIG * BIG + NSMALL * SMALL
        dma, vmem = pltpu.SemaphoreType.DMA, pltpu.VMEM
        return pl.pallas_call(
            functools.partial(kernel, d, f),
            out_shape=jax.ShapeDtypeStruct((rows, d), BF16),
            in_specs=[pl.BlockSpec(memory_space=pltpu.HBM)] * 4,
            out_specs=pl.BlockSpec(memory_space=pltpu.HBM),
            scratch_shapes=[
                vmem((2, BIG, d), BF16),
                vmem((2, BIG, f), BF16),
                vmem((2, d, 2 * T), BF16),
                vmem((2, f, 2 * T), BF16),
                vmem((BIG, 2 * T), F32),
                vmem((N_OWN + 1, R, T), F32),
                vmem((N_PRECV + 1, R, T), BF16),
                vmem((N_RO + 1, R, T), BF16),
                vmem((N_RI + 1, H, T), BF16),
                vmem((N_PS, R, T), BF16),
                vmem((N_AS + 1, R, T), BF16),
                vmem((N_FS + 1, H, T), BF16),
                dma((2, 4)),
                dma((2,)),
                dma((N_PS,)),
                dma((N_PRECV,)),
                dma((N_AS,)),
                dma((N_RO,)),
                dma((N_RI,)),
                dma((N_FS, 4)),
                dma((N_Y,)),
                dma((N_Y,)),
                dma,
                dma,
            ],
            compiler_params=pltpu.CompilerParams(
                collective_id=0, has_side_effects=True, vmem_limit_bytes=67043328
            ),
            name="mlp",
        )(x, w_gate, w_up, w_down)

    return jax.shard_map(
        step,
        mesh=mesh,
        in_specs=(P("dp", None), P(None, "tp"), P(None, "tp"), P("tp", None)),
        out_specs=P("dp", None),
        check_vma=False,
    )
```

```python
import functools

import jax
import jax.numpy as jnp
from jax import lax
from jax.experimental import pallas as pl
from jax.experimental.pallas import tpu as pltpu
from jax.sharding import PartitionSpec as P

MESH = pl.DeviceIdType.MESH
BF16, F32 = jnp.bfloat16, jnp.float32

T = 256
R = 256
H = R // 2
BIG, SMALL = 512, 256
NBIG, NSMALL = 3, 2
N_OWN, N_PRECV, N_RO, N_RI, N_PS, N_AS, N_FS, N_Y = 13, 10, 11, 11, 4, 8, 8, 14
FAR = {"p": 2, "ao": 2, "ai": 5, "f": 8, "y1": 12, "y2": 15}
WIDE = {"p": 2, "ao": 2, "ai": 7, "f": 12, "y1": 17, "y2": 20}
NEAR = {"p": 2, "ao": 2, "ai": 4, "f": 6, "y1": 8, "y2": 10}


def kernel(
    d, f, x, wg, wu, wd, y,
    xb, hid, wgu, wdb, gu, own, precv, ro, ri, ps, asd, fs,
    wsem, xsem, ps_sem, precv_sem, as_sem, ro_sem, ri_sem, fs_sem, ya_sem, yb_sem, yp_sem, fw_sem,
):
    half = d // 2
    steps = f // T
    assert half // T == steps
    n_units = steps * (NBIG * BIG + NSMALL * SMALL) // R
    per_big = BIG // R
    big_units = NBIG * steps * per_big

    tp = lax.axis_index("tp")
    z, c = lax.div(tp, 2), lax.rem(tp, 2)
    inner = jnp.logical_and(z >= 1, z <= 2)
    outer = jnp.logical_not(inner)
    partner = {"tp": z * 2 + 1 - c}
    near = 1 + lax.div(z, 2)
    to_near = {"tp": near * 2 + c}
    to_inner = {"tp": (3 - near) * 2 + c}
    to_outer = {"tp": 3 * (near - 1) * 2 + c}
    near_rows = (near - 1) * H
    far_rows = (2 - near) * H
    my_cols, other_cols = c * half, (1 - c) * half

    def remote(src, dst, send, recv, dev):
        return pltpu.make_async_remote_copy(
            src_ref=src, dst_ref=dst, send_sem=send, recv_sem=recv, device_id=dev, device_id_type=MESH
        )

    def valid(v):
        return jnp.logical_and(v >= 0, v < n_units)

    def slot(v, n):
        return jnp.where(valid(v), lax.rem(v + 64 * n, n), n)

    def unit_at(v):
        b = jnp.where(v < big_units, 1, 0)
        w = v - big_units
        row_b = lax.div(v, steps * per_big) * BIG + lax.rem(v, per_big) * R
        col_b = lax.div(lax.rem(v, steps * per_big), per_big) * T
        row_s = NBIG * BIG + lax.div(w, steps) * SMALL
        col_s = lax.rem(w, steps) * T
        row = b * row_b + (1 - b) * row_s
        col = b * col_b + (1 - b) * col_s
        return row, col

    def y_at(v, rows):
        row, col = unit_at(v)
        return y.at[pl.ds(pl.multiple_of(row + rows, H), H), pl.ds(pl.multiple_of(my_cols + col, T), T)]

    def g_copies(j, s):
        cols = pl.ds(pl.multiple_of(j * T, T), T)
        return [
            pltpu.make_async_copy(wg.at[:, cols], wgu.at[s, :, pl.ds(0, T)], wsem.at[s, 0]),
            pltpu.make_async_copy(wu.at[:, cols], wgu.at[s, :, pl.ds(T, T)], wsem.at[s, 1]),
        ]

    def d_copies(j, s):
        theirs = pl.ds(pl.multiple_of(other_cols + j * T, T), T)
        mine = pl.ds(pl.multiple_of(my_cols + j * T, T), T)
        return [
            pltpu.make_async_copy(wd.at[:, theirs], wdb.at[s, :, pl.ds(0, T)], wsem.at[s, 2]),
            pltpu.make_async_copy(wd.at[:, mine], wdb.at[s, :, pl.ds(T, T)], wsem.at[s, 3]),
        ]

    def x_copy(row, rows, s):
        return pltpu.make_async_copy(x.at[pl.ds(row, rows)], xb.at[s, pl.ds(0, rows)], xsem.at[s])

    def start(copies):
        for cp in copies:
            cp.start()

    def wait(copies):
        for cp in copies:
            cp.wait()

    def ps_copy(v):
        s = lax.rem(v, N_PS)
        return remote(ps.at[s], precv.at[lax.rem(v, N_PRECV)], ps_sem.at[s], precv_sem.at[lax.rem(v, N_PRECV)], partner)

    def ps_free(v):
        @pl.when(v >= N_PS)
        def _():
            ps_copy(v - N_PS).wait_send()

    def p_wait(v):
        @pl.when(valid(v))
        def _():
            ps_copy(v).wait_recv()

    def ao_copy(v):
        s = lax.rem(v, N_AS)
        return remote(asd.at[s], ro.at[lax.rem(v, N_RO)], as_sem.at[s], ro_sem.at[lax.rem(v, N_RO)], to_near)

    def ai_copy(v):
        s = lax.rem(v, N_AS)
        rows = pl.ds(pl.multiple_of(far_rows, H), H)
        return remote(asd.at[s, rows], ri.at[lax.rem(v, N_RI)], as_sem.at[s], ri_sem.at[lax.rem(v, N_RI)], to_inner)

    def a_wait(v):
        @pl.when(jnp.logical_and(outer, jnp.logical_and(v >= N_AS, v < n_units)))
        def _():
            ao_copy(v - N_AS).wait_send()

        @pl.when(jnp.logical_and(inner, jnp.logical_and(v >= N_AS, v < n_units)))
        def _():
            ai_copy(v - N_AS).wait_send()

        @pl.when(jnp.logical_and(inner, valid(v)))
        def _():
            ao_copy(v).wait_recv()

    def a_compute(v):
        so = slot(v, N_OWN)
        sr = jnp.where(inner, slot(v, N_RO), N_RO)
        total = own[so] + precv[slot(v, N_PRECV)].astype(F32) + ro[sr].astype(F32)
        own[so] = total
        asd[slot(v, N_AS)] = total.astype(BF16)

    def a_start(v):
        @pl.when(jnp.logical_and(outer, valid(v)))
        def _():
            ao_copy(v).start()

        @pl.when(jnp.logical_and(inner, valid(v)))
        def _():
            ai_copy(v).start()

    def f_copies(v):
        s = lax.rem(v, N_FS)
        at = y_at(v, near_rows)
        ys = lax.rem(v, N_Y)
        return [
            remote(fs.at[s], at, fs_sem.at[s, 0], ya_sem.at[ys], to_outer),
            remote(fs.at[s], at, fs_sem.at[s, 1], ya_sem.at[ys], to_inner),
            remote(fs.at[s], at, fs_sem.at[s, 2], yp_sem, partner),
            pltpu.make_async_copy(fs.at[s], at, fs_sem.at[s, 3]),
        ]

    def f_wait_sends(v):
        copies = f_copies(v)
        for cp in copies[:3]:
            cp.wait_send()
        copies[3].wait()

    def f_wait(v):
        @pl.when(jnp.logical_and(inner, jnp.logical_and(v >= N_FS, v < n_units)))
        def _():
            f_wait_sends(v - N_FS)

        @pl.when(jnp.logical_and(inner, valid(v)))
        def _():
            ai_copy(v).wait_recv()

    def f_compute(v):
        v = jnp.where(inner, v, -1)
        rows = pl.ds(pl.multiple_of(near_rows, H), H)
        fs[slot(v, N_FS)] = (own[slot(v, N_OWN), rows, :] + ri[slot(v, N_RI)].astype(F32)).astype(BF16)

    def f_start(v):
        @pl.when(jnp.logical_and(inner, valid(v)))
        def _():
            start(f_copies(v))

    def y1(v):
        @pl.when(jnp.logical_and(inner, valid(v)))
        def _():
            at = y_at(v, far_rows)
            remote(at, at, fw_sem, ya_sem.at[lax.rem(v, N_Y)], to_inner).wait_recv()
            remote(at, at, fw_sem, yb_sem.at[lax.rem(v, N_Y)], to_outer).start()
            remote(at, at, fw_sem, yp_sem, partner).start()

        @pl.when(jnp.logical_and(outer, valid(v)))
        def _():
            at = y_at(v, near_rows)
            remote(at, at, fw_sem, ya_sem.at[lax.rem(v, N_Y)], to_near).wait_recv()
            remote(at, at, fw_sem, yp_sem, partner).start()

    def y2(v):
        @pl.when(jnp.logical_and(outer, valid(v)))
        def _():
            at = y_at(v, far_rows)
            remote(at, at, fw_sem, yb_sem.at[lax.rem(v, N_Y)], to_near).wait_recv()
            remote(at, at, fw_sem, yp_sem, partner).start()

    def stages(at):
        p_wait(at["p"])
        a_wait(at["a"])

        @pl.when(valid(at["a"]))
        def _():
            a_compute(at["a"])

        a_start(at["a"])
        f_wait(at["f"])

        @pl.when(jnp.logical_and(inner, valid(at["f"])))
        def _():
            f_compute(at["f"])

        f_start(at["f"])
        y1(at["y1"])
        y2(at["y2"])

    def waits(ats):
        for fn, key in ((p_wait, "p"), (a_wait, "a"), (f_wait, "f"), (y1, "y1"), (y2, "y2")):
            for at in ats:
                fn(at[key])

    def computes(ats):
        for at in ats:
            a_compute(at["a"])
        for at in ats:
            f_compute(at["f"])

    def starts(ats):
        for at in ats:
            a_start(at["a"])
        for at in ats:
            f_start(at["f"])

    def by_role(lags):
        return {"p": lags["p"], "a": jnp.where(inner, lags["ai"], lags["ao"]), "f": lags["f"], "y1": lags["y1"], "y2": lags["y2"]}

    far, wide, near_end = by_role(FAR), by_role(WIDE), by_role(NEAR)

    def behind(u, lags):
        return {k: u - v for k, v in lags.items()}

    def opening(base, q):
        turns = steps * per_big
        at = {}
        for k in far:
            now = q - lax.div(q * (wide[k] - far[k]), turns)
            then = q + 1 - lax.div((q + 1) * (wide[k] - far[k]), turns)
            at[k] = jnp.where(then == now, -1, base - far[k] + now)
        return at

    def closing(base, j):
        return {k: base - wide[k] + j + lax.div(j * (wide[k] - near_end[k]), steps) for k in wide}

    def epilogue(rows, s, j):
        g, u = gu[pl.ds(0, rows), pl.ds(0, T)], gu[pl.ds(0, rows), pl.ds(T, T)]
        h = (g * jax.nn.sigmoid(g) * u).astype(BF16)
        hid[s, pl.ds(0, rows), pl.ds(pl.multiple_of(j * T, T), T)] = h

    def gate_up(rows, s, w):
        gu[pl.ds(0, rows), :] = jnp.dot(xb[s, pl.ds(0, rows)], wgu[w], preferred_element_type=F32)

    def down(rows, s, w, u0):
        t = jnp.dot(hid[s, pl.ds(0, rows)], wdb[w], preferred_element_type=F32)
        for i in range(rows // R):
            part = t[i * R : (i + 1) * R]
            ps[lax.rem(u0 + i, N_PS)] = part[:, :T].astype(BF16)
            own[lax.rem(u0 + i, N_OWN)] = part[:, T:]

    def two_units(rows, sd, sg, w, j, u0, ats):

        @pl.when(j == 0)
        def _():
            epilogue(BIG, sd, steps - 1)

        for i in range(per_big):
            ps_free(u0 + i)
        waits(ats[:1])
        wait(d_copies(j, w))
        computes(ats[:1])
        down(BIG, sd, w, u0)
        for i in range(per_big):
            ps_copy(u0 + i).start()
        starts(ats[:1])
        waits(ats[1:])
        wait(g_copies(j, w))
        epilogue(rows, jnp.where(j == 0, sd, sg), lax.rem(j + steps - 1, steps))
        computes(ats[1:])
        gate_up(rows, sg, w)
        starts(ats[1:])

    barrier = pltpu.get_barrier_semaphore()
    x_copy(0, BIG, 0).start()
    start(g_copies(0, 0))
    pl.semaphore_signal(barrier, inc=1, device_id=partner, device_id_type=MESH)

    @pl.when(outer)
    def _():
        pl.semaphore_signal(barrier, inc=1, device_id=to_near, device_id_type=MESH)

    @pl.when(inner)
    def _():
        pl.semaphore_signal(barrier, inc=1, device_id=to_outer, device_id_type=MESH)
        pl.semaphore_signal(barrier, inc=1, device_id=to_inner, device_id_type=MESH)

    gu[...] = jnp.zeros_like(gu)
    ro[N_RO] = jnp.zeros((R, T), BF16)
    x_copy(0, BIG, 0).wait()

    def first(j, _):
        w = lax.rem(j, 2)

        @pl.when(j < steps - 1)
        def _():
            start(g_copies(j + 1, 1 - w))

        @pl.when(j == steps - 1)
        def _():
            start(g_copies(0, 1 - w))
            start(d_copies(0, 1 - w))

        @pl.when(j == 1)
        def _():
            x_copy(BIG, BIG, 1).start()

        wait(g_copies(j, w))
        epilogue(BIG, 0, lax.rem(j + steps - 1, steps))
        gate_up(BIG, 0, w)
        return 0

    lax.fori_loop(0, steps, first, 0)

    @pl.when(outer)
    def _():
        pl.semaphore_wait(barrier, 2)

    @pl.when(inner)
    def _():
        pl.semaphore_wait(barrier, 3)

    def both(t, _):
        k, j = lax.div(t, steps), lax.rem(t, steps)
        w = lax.rem(t, 2)
        sd, sg = lax.rem(k, 2), lax.rem(k + 1, 2)
        u0 = t * per_big
        jn = lax.rem(j + 1, steps)
        start(g_copies(jn, 1 - w))
        start(d_copies(jn, 1 - w))

        @pl.when(j == 0)
        def _():
            x_copy(0, BIG, sg).wait()

        for kk in range(NBIG - 1):
            rows = BIG if kk + 2 < NBIG else SMALL

            @pl.when(t == kk * steps + 1)
            def _():
                x_copy((kk + 2) * BIG, rows, kk % 2).start()

        two_units(BIG, sd, sg, w, j, u0, [behind(u0 + i, far) for i in range(per_big)])
        return 0

    lax.fori_loop(0, steps * (NBIG - 1), both, 0)

    for k in range(NBIG - 1, NBIG + NSMALL - 1):
        r = per_big if k < NBIG else 1
        base = (NBIG - 1) * steps * per_big if k < NBIG else big_units + (k - NBIG) * steps
        sd, sg = k % 2, (k + 1) % 2
        last = k == NBIG + NSMALL - 2
        x_copy(0, SMALL, sg).wait()

        def small(j, _, r=r, base=base, sd=sd, sg=sg, last=last, k=k):
            w = lax.rem(j, 2)
            u0 = base + j * r
            jn = lax.rem(j + 1, steps)
            if last:

                @pl.when(j < steps - 1)
                def _():
                    start(g_copies(jn, 1 - w))
            else:
                start(g_copies(jn, 1 - w))
            start(d_copies(jn, 1 - w))
            if not last:

                @pl.when(j == 1)
                def _():
                    x_copy(NBIG * BIG + (k + 2 - NBIG) * SMALL, SMALL, sd).start()

            if k < NBIG:
                two_units(SMALL, sd, sg, w, j, u0, [opening(base, j * r + i) for i in range(r)])
                return 0

            @pl.when(j == 0)
            def _():
                epilogue(SMALL, sd, steps - 1)

            one, two = closing(base, j), closing(base, j + 1)
            stages({a: jnp.where(two[a] - one[a] == 2, one[a], -1) for a in one})
            ats = [{a: two[a] - 1 for a in two}]
            ps_free(u0)
            waits(ats)
            wait(d_copies(j, w))
            computes(ats)
            down(SMALL, sd, w, u0)
            ps_copy(u0).start()
            starts(ats)
            wait(g_copies(j, w))
            epilogue(SMALL, jnp.where(j == 0, sd, sg), lax.rem(j + steps - 1, steps))
            gate_up(SMALL, sg, w)
            return 0

        lax.fori_loop(0, steps, small, 0)

    sd = (NBIG + NSMALL - 1) % 2
    epilogue(SMALL, sd, steps - 1)

    def final(j, _):
        w = lax.rem(j, 2)
        u0 = n_units - steps + j

        @pl.when(j < steps - 1)
        def _():
            start(d_copies(j + 1, 1 - w))

        stages(behind(u0, near_end))
        ps_free(u0)
        wait(d_copies(j, w))
        down(SMALL, sd, w, u0)
        ps_copy(u0).start()
        return 0

    lax.fori_loop(0, steps, final, 0)

    def drain(i, _):
        stages(behind(n_units + i, near_end))
        return 0

    lax.fori_loop(0, NEAR["y2"], drain, 0)

    for v in range(n_units - N_PS, n_units):
        ps_copy(v).wait_send()

    @pl.when(outer)
    def _():
        for v in range(n_units - N_AS, n_units):
            ao_copy(v).wait_send()

    @pl.when(inner)
    def _():
        for v in range(n_units - N_AS, n_units):
            ai_copy(v).wait_send()
        for v in range(n_units - N_FS, n_units):
            f_wait_sends(v)

    sent = y.at[:, pl.ds(pl.multiple_of(my_cols, T), half)]
    got = y.at[:, pl.ds(pl.multiple_of(other_cols, T), half)]
    remote(sent, got, fw_sem, yp_sem, partner).wait_send()
    remote(sent, got, fw_sem, yp_sem, partner).wait_recv()


def solution(mesh):
    def step(x, w_gate, w_up, w_down):
        d, f = w_gate.shape
        rows = x.shape[0]
        assert rows == NBIG * BIG + NSMALL * SMALL
        dma, vmem = pltpu.SemaphoreType.DMA, pltpu.VMEM
        return pl.pallas_call(
            functools.partial(kernel, d, f),
            out_shape=jax.ShapeDtypeStruct((rows, d), BF16),
            in_specs=[pl.BlockSpec(memory_space=pltpu.HBM)] * 4,
            out_specs=pl.BlockSpec(memory_space=pltpu.HBM),
            scratch_shapes=[
                vmem((2, BIG, d), BF16),
                vmem((2, BIG, f), BF16),
                vmem((2, d, 2 * T), BF16),
                vmem((2, f, 2 * T), BF16),
                vmem((BIG, 2 * T), F32),
                vmem((N_OWN + 1, R, T), F32),
                vmem((N_PRECV + 1, R, T), BF16),
                vmem((N_RO + 1, R, T), BF16),
                vmem((N_RI + 1, H, T), BF16),
                vmem((N_PS, R, T), BF16),
                vmem((N_AS + 1, R, T), BF16),
                vmem((N_FS + 1, H, T), BF16),
                dma((2, 4)),
                dma((2,)),
                dma((N_PS,)),
                dma((N_PRECV,)),
                dma((N_AS,)),
                dma((N_RO,)),
                dma((N_RI,)),
                dma((N_FS, 4)),
                dma((N_Y,)),
                dma((N_Y,)),
                dma,
                dma,
            ],
            compiler_params=pltpu.CompilerParams(
                collective_id=0, has_side_effects=True, vmem_limit_bytes=67043328
            ),
            name="mlp",
        )(x, w_gate, w_up, w_down)

    return jax.shard_map(
        step,
        mesh=mesh,
        in_specs=(P("dp", None), P(None, "tp"), P(None, "tp"), P("tp", None)),
        out_specs=P("dp", None),
        check_vma=False,
    )
```
